32 devices in a mesh: ba: 8 (over z, y), dev: 4 (over x, core).
Axes of the slice: x: 2, y: 2, z: 4, core: 2. Of those that a mesh axis runs over, the one named last changes fastest.
Arguments:
- factors: bfloat16 [16, 512, 1024], P('ba', 'dev'), may hold values from -0.1875 to 0.1875
- amplitudes: bfloat16 [64, 512, 512], P(None, 'dev'), may hold values from -0.375 to 0.375
- pair_order: int32 [64], replicated, may hold values from 0 to 63, each once
- occ_bin: int32 [8], replicated, may hold values from 0 to 127
- vir_bin: int32 [16], replicated, may hold values from 0 to 127
- levels: float32 [128], replicated, may hold values from 0.1 to 0.8
Outputs:
- update: float32 [16, 1024], P('ba', 'dev')
The draws below stay inside these ranges and needn't reach their ends.
Inputs may be any that keep to these rules, and one draw needn't show every extreme that they name: `pair_order`: each value appears once; entry k names the ordered occupied pair (value // 8, value % 8). `occ_bin`: orbital i has energy minus levels at its bin. `vir_bin`: window virtual a has energy levels at its bin.
All inputs are finite; a program needn't handle non-finite values.
Results may differ from the reference program's by a relative error of at most 0.0029.
Values may be sent and summed in bfloat16 or wider, within the bound.
A program may use at most 64 MiB of HBM per device.

```python
import jax
import jax.numpy as jnp
from jax import lax

V = 512
NAUX = 1024
NOCC = 8
LEVELS = 128
NW = 16
P_SIZE = 64


def touch_ends(entries, own_key, low, largest):
    longest = entries.shape.index(max(entries.shape))
    spots = []
    for shift in (0, 1):
        where = [jax.random.randint(jax.random.fold_in(own_key, axis), (), 0, length) for axis, length in enumerate(entries.shape)]
        where[longest] = (where[longest] + shift) % entries.shape[longest]
        spots.append(tuple(where))
    return entries.at[spots[0]].set(low).at[spots[1]].set(largest)


def steps_of(key, dims, pieces, least, largest):
    loudness, own = 1.0, jax.random.fold_in(key, 6)
    for axis_at, blocks in pieces:
        draws = jnp.exp(jax.random.uniform(jax.random.fold_in(own, axis_at), (blocks,), jnp.float32, least / len(pieces), largest / len(pieces)))
        loudness = loudness * jnp.repeat(draws, dims[axis_at] // blocks).reshape([-1 if axis == axis_at else 1 for axis in range(len(dims))])
    return loudness


def bell_draw(rng, shape, deviation, bound, shards=(), kind=jnp.bfloat16):
    factor_of = steps_of(rng, shape, shards, -0.22, 0.18) if shards else 1.0
    array = jax.random.normal(rng, shape, jnp.float32) * deviation * factor_of
    return jnp.minimum(jnp.maximum(array, -bound), bound).astype(kind)


def setup_inputs(seed: int = 0) -> dict:
    splits = jax.random.split(jax.random.key(seed), 7)
    factors = bell_draw(splits[0], (NW, V, NAUX), NAUX ** -0.5, 0.1875, ((0, 8), (1, 4)))
    amplitudes = bell_draw(splits[1], (P_SIZE, V, V), (V * V // NAUX) ** -0.5, 0.375, ((1, 4),))
    pair_order = jax.random.permutation(splits[2], P_SIZE).astype(jnp.int32)
    occ_bin = touch_ends(jax.random.randint(splits[3], (NOCC,), 0, LEVELS), jax.random.fold_in(splits[3], 1), 0, LEVELS - 1).astype(jnp.int32)
    vir_bin = touch_ends(jax.random.randint(splits[4], (NW,), 0, LEVELS), jax.random.fold_in(splits[4], 1), 0, LEVELS - 1).astype(jnp.int32)
    levels = jnp.clip(jax.random.uniform(splits[5], (LEVELS,), jnp.float32, 0.1, 0.8), 0.1, 0.8)
    return {"factors": factors, "amplitudes": amplitudes, "pair_order": pair_order, "occ_bin": occ_bin, "vir_bin": vir_bin, "levels": levels}


level_shift = 0.3


def reference(factors, amplitudes, pair_order, occ_bin, vir_bin, levels):
    flat_rows = factors.reshape(NW * V, NAUX)
    flat_amps = amplitudes.reshape(P_SIZE, V * V)

    def one_column(slab):
        integrals = lax.dot_general(flat_rows, slab, (((1,), (1,)), ((), ())), preferred_element_type=jnp.float32)
        integrals = integrals.astype(jnp.bfloat16).reshape(NW, V * V)
        return lax.dot_general(integrals, flat_amps, (((1,), (1,)), ((), ())), preferred_element_type=jnp.float32)

    ladder = lax.map(one_column, factors)
    counter = jnp.arange(P_SIZE, dtype=jnp.int32)
    swapped = (pair_order % NOCC) * NOCC + pair_order // NOCC
    matches = swapped[:, None] == pair_order[None, :]
    partner = jnp.sum(jnp.where(matches, counter[None, :], 0), axis=1).astype(jnp.int32)
    total = ladder + jnp.transpose(ladder, (1, 0, 2))[:, :, partner]
    virtual_energy = levels[vir_bin]
    occupied_energy = -levels[occ_bin]
    pair_energy = occupied_energy[pair_order // NOCC] + occupied_energy[pair_order % NOCC]
    denominator = virtual_energy[:, None, None] + virtual_energy[None, :, None] - pair_energy[None, None, :] + level_shift
    return (total / denominator).reshape(NW, NW * P_SIZE)
```

```python
import functools

import jax
import jax.numpy as jnp
from jax import lax
from jax.experimental import pallas as pl
from jax.experimental.pallas import tpu as pltpu
from jax.sharding import PartitionSpec as P

NOCC = 8
LANES = 128
MESH = pl.DeviceIdType.MESH

level_shift = 0.3


def flip_bits(index, bits):
    result = index
    bit = 1
    while bit <= bits:
        if bits & bit:
            result = result + bit - 2 * bit * ((result // bit) % 2)
        bit *= 2
    return result


def to_column(row):
    n = row.shape[1]
    rows = lax.broadcasted_iota(jnp.int32, (n, n), 0)
    lanes = lax.broadcasted_iota(jnp.int32, (n, n), 1)
    return jnp.sum(jnp.where(rows == lanes, row, jnp.zeros_like(row)), axis=1, keepdims=True)


def kernel(
    dims,
    f_hbm,
    amps_hbm,
    order_ref,
    occ_ref,
    vir_ref,
    levels_ref,
    out_ref,
    local,
    right,
    other,
    left_f32,
    left,
    raw,
    stage,
    amps,
    ints,
    acc,
    tiles,
    parts,
    load_sem,
    own_sem,
    amp_sem,
    send_z,
    send_o,
    send_c,
    send_y,
    recv_piece,
    recv_y,
    send_f,
    recv_f,
):
    nz, ny, no, owned, cols, qs, window, pairs, virt, tile_c, amp_c = dims
    nd = no * 2
    nb = nz * owned
    total = nz * ny * nd
    split = window // nd
    ba, dev = lax.axis_index("ba"), lax.axis_index("dev")
    me = ba * nd + dev
    z, y = ba // ny, ba % ny
    outer, core = dev // 2, dev % 2
    partner_core = outer * 2 + 1 - core
    chunks = cols // amp_c

    load = pltpu.make_async_copy(f_hbm, local, load_sem)
    load.start()
    own = pltpu.make_async_copy(
        f_hbm.at[:, :, pl.ds(pl.multiple_of(z * qs, LANES), qs)], right.at[z, :, dev], own_sem
    )
    own.start()

    def amp_load(chunk):
        return pltpu.make_async_copy(
            amps_hbm.at[:, pl.ds(chunk * amp_c, amp_c), :], raw.at[chunk], amp_sem.at[chunk]
        )

    for chunk in range(chunks):
        amp_load(chunk).start()

    barrier = pltpu.get_barrier_semaphore()

    def greet(step, carry):
        there = (me + step) % total
        pl.semaphore_signal(
            barrier, inc=1, device_id=(there // nd, there % nd), device_id_type=MESH
        )
        return carry

    lax.fori_loop(1, total, greet, 0)
    load.wait()
    own.wait()
    pl.semaphore_wait(barrier, total - 1)

    def piece_copy(piece_z, piece_d, send, ba_to, dev_to):
        return pltpu.make_async_remote_copy(
            src_ref=right.at[piece_z, :, piece_d],
            dst_ref=right.at[piece_z, :, piece_d],
            send_sem=send,
            recv_sem=recv_piece.at[piece_z, piece_d],
            device_id=(ba_to, dev_to),
            device_id_type=MESH,
        )

    pending = []
    for step in range(1, nz):
        there = flip_bits(z, step)
        copy = pltpu.make_async_remote_copy(
            src_ref=local.at[:, :, pl.ds(pl.multiple_of(there * qs, LANES), qs)],
            dst_ref=right.at[z, :, dev],
            send_sem=send_z.at[step],
            recv_sem=recv_piece.at[z, dev],
            device_id=(there * ny + y, dev),
            device_id_type=MESH,
        )
        copy.start()
        pending.append(copy)

    def forward(step):
        from_z = flip_bits(z, step)
        if step:
            piece_copy(from_z, dev, send_z.at[0], ba, partner_core).wait_recv()
        for other_outer in range(1, no):
            copy = piece_copy(
                from_z,
                dev,
                send_o.at[step, other_outer],
                ba,
                flip_bits(outer, other_outer) * 2 + core,
            )
            copy.start()
            pending.append(copy)
        for other_y in range(1, ny):
            copy = pltpu.make_async_remote_copy(
                src_ref=right.at[from_z, :, dev],
                dst_ref=other.at[y, from_z],
                send_sem=send_y.at[step, other_y],
                recv_sem=recv_y.at[y, from_z],
                device_id=(z * ny + flip_bits(y, other_y), dev),
                device_id_type=MESH,
            )
            copy.start()
            pending.append(copy)
        copy = piece_copy(from_z, dev, send_c.at[step, 0], ba, partner_core)
        copy.start()
        pending.append(copy)

    def widen(source, at_y, at_z):
        for i in range(owned):
            row = (at_z * ny + at_y) * owned + i
            base = pl.multiple_of(row * (cols + 8), 8)
            for h in range(qs // LANES):
                left_f32[h, pl.ds(base, cols), :] = source[
                    i, :, h * LANES : (h + 1) * LANES
                ].astype(jnp.float32)

    def amp_chunk(chunk):
        amp_load(chunk).wait()
        pitch = amp_c + 8

        def spread(k, carry):
            base = pl.multiple_of(k * pitch, 8)
            for h in range(virt // LANES):
                stage[h, pl.ds(base, amp_c), :] = raw[
                    chunk, k, :, h * LANES : (h + 1) * LANES
                ].astype(jnp.float32)
            return carry

        lax.fori_loop(0, pairs, spread, 0, unroll=4)

        def gather(c, carry):
            for h in range(virt // LANES):
                amps[chunk * amp_c + c, :, h * LANES : (h + 1) * LANES] = stage[
                    h, pl.ds(c, pairs, stride=pitch), :
                ].astype(jnp.bfloat16)
            return carry

        lax.fori_loop(0, amp_c, gather, 0)

    done = 0
    for step in range(nz):
        forward(step)
        upto = (step + 1) * chunks // nz
        for chunk in range(done, upto):
            amp_chunk(chunk)
        done = upto
        from_z = flip_bits(z, step)
        widen(right.at[from_z, :, dev], y, from_z)

    for step in range(nz):
        from_z = flip_bits(z, step)
        for other_outer in range(1, no):
            from_d = flip_bits(outer, other_outer) * 2 + core
            piece_copy(from_z, from_d, send_z.at[0], ba, partner_core).wait_recv()
            copy = piece_copy(from_z, from_d, send_c.at[step, other_outer], ba, partner_core)
            copy.start()
            pending.append(copy)
        for other_y in range(1, ny):
            from_y = flip_bits(y, other_y)
            pltpu.make_async_remote_copy(
                src_ref=right.at[from_z, :, dev],
                dst_ref=other.at[from_y, from_z],
                send_sem=send_z.at[0],
                recv_sem=recv_y.at[from_y, from_z],
                device_id=(ba, partner_core),
                device_id_type=MESH,
            ).wait_recv()
            widen(other.at[from_y, from_z], from_y, from_z)

    def turn(c, carry):
        rows = pl.ds(pl.multiple_of(c * window, window), window)
        for h in range(qs // LANES):
            left[rows, h * LANES : (h + 1) * LANES] = left_f32[
                h, pl.ds(c, window, stride=cols + 8), :
            ].astype(jnp.bfloat16)
        return carry

    lax.fori_loop(0, cols, turn, 0, unroll=4)

    for step in range(nz):
        from_z = flip_bits(z, step)
        for other_outer in range(no):
            from_d = flip_bits(outer, other_outer) * 2 + 1 - core
            piece_copy(from_z, from_d, send_z.at[0], ba, partner_core).wait_recv()

    acc[...] = jnp.zeros_like(acc)
    block = tile_c * window

    def contract(ct, carry):
        rows = left[pl.ds(pl.multiple_of(ct * block, block), block), :]
        for b in range(nb):
            side = right[b // owned, b % owned].reshape(virt, qs)
            part = lax.dot_general(
                rows, side, (((1,), (1,)), ((), ())), preferred_element_type=jnp.float32
            )
            ints[:, b * window : (b + 1) * window, :] = part.astype(jnp.bfloat16).reshape(
                tile_c, window, virt
            )

        def add(t, value):
            return value + lax.dot_general(
                ints[t],
                amps[ct * tile_c + t],
                (((1,), (1,)), ((), ())),
                preferred_element_type=jnp.float32,
            )

        acc[:, :, 0:pairs] += lax.fori_loop(
            0, tile_c, add, jnp.zeros((nb * window, pairs), jnp.float32), unroll=4
        ).reshape(nb, window, pairs)
        return carry

    lax.fori_loop(0, cols // tile_c, contract, 0)
    acc[:, :, pairs : 2 * pairs] = acc[:, :, 0:pairs]

    height = owned * split
    row_at = lax.broadcasted_iota(jnp.int32, (height, 2 * pairs), 0)
    lane_at = lax.broadcasted_iota(jnp.int32, (height, 2 * pairs), 1)

    def make_tile(there):
        to_ba, to_dev = there // nd, there % nd
        to_z, to_y = to_ba // ny, to_ba % ny
        straight = jnp.zeros((height, 2 * pairs), jnp.float32)
        pieces = []
        turned = []
        for i in range(owned):
            pieces.append(acc[to_z * owned + i, pl.ds(to_dev * split, split), :])
            for a in range(split):
                row = to_dev * split + a
                owner = row // owned
                turned.append(
                    acc[(owner // ny) * owned + row % owned, pl.ds(to_ba * owned + i, 1), :]
                )
        straight = jnp.concatenate(pieces, axis=0)
        flipped = jnp.concatenate(turned, axis=0)
        same = jnp.zeros((height, 2 * pairs), jnp.int32) + to_y == y
        owner_at = (to_dev * split + row_at % split) // owned
        return jnp.where(
            lane_at < pairs,
            jnp.where(same, straight, 0.0),
            jnp.where(owner_at % ny == y, flipped, 0.0),
        )

    def tile_copy(there):
        return pltpu.make_async_remote_copy(
            src_ref=tiles.at[there],
            dst_ref=parts.at[me],
            send_sem=send_f.at[there],
            recv_sem=recv_f.at[me],
            device_id=(there // nd, there % nd),
            device_id_type=MESH,
        )

    def send_tile(step, carry):
        there = (me + step) % total
        tiles[there] = make_tile(there)
        tile_copy(there).start()
        return carry

    lax.fori_loop(1, total, send_tile, 0)
    parts[me] = make_tile(me)

    levels = to_column(levels_ref[...])
    level_at = lax.broadcasted_iota(jnp.int32, (levels.shape[0], window), 0)
    virtual = jnp.sum(
        jnp.where(level_at == vir_ref[...], levels, 0.0), axis=0, keepdims=True
    )
    level_occ = lax.broadcasted_iota(jnp.int32, (levels.shape[0], NOCC), 0)
    occupied = to_column(
        -jnp.sum(jnp.where(level_occ == occ_ref[...], levels, 0.0), axis=0, keepdims=True)
    )
    order = order_ref[...]
    first, second = order // NOCC, order % NOCC
    occ_at = lax.broadcasted_iota(jnp.int32, (NOCC, pairs), 0)
    pair_energy = jnp.sum(
        jnp.where(occ_at == first, occupied, 0.0), axis=0, keepdims=True
    ) + jnp.sum(jnp.where(occ_at == second, occupied, 0.0), axis=0, keepdims=True)
    win_row = lax.broadcasted_iota(jnp.int32, (height, window), 0)
    win_lane = lax.broadcasted_iota(jnp.int32, (height, window), 1)
    right_energy = jnp.sum(
        jnp.where(win_lane == ba * owned + win_row // split, virtual, 0.0), axis=1, keepdims=True
    )
    left_energy = jnp.sum(
        jnp.where(win_lane == dev * split + win_row % split, virtual, 0.0), axis=1, keepdims=True
    )
    denominator = right_energy + left_energy - pair_energy + level_shift
    permuter = (to_column(order) == second * NOCC + first).astype(jnp.float32)

    def arrive(step, carry):
        there = (me + step) % total
        pltpu.make_async_remote_copy(
            src_ref=tiles.at[there],
            dst_ref=parts.at[there],
            send_sem=send_f.at[there],
            recv_sem=recv_f.at[there],
            device_id=(there // nd, there % nd),
            device_id_type=MESH,
        ).wait_recv()
        return carry

    lax.fori_loop(1, total, arrive, 0)
    summed = jnp.sum(parts[...], axis=0)
    moved = jnp.dot(
        summed[:, pairs:],
        permuter,
        precision=lax.Precision.HIGHEST,
        preferred_element_type=jnp.float32,
    )
    result = (summed[:, :pairs] + moved) / denominator
    for i in range(owned):
        for a in range(split):
            out_ref[i : i + 1, a * pairs : (a + 1) * pairs] = result[
                i * split + a : i * split + a + 1, :
            ]

    for copy in pending:
        copy.wait_send()

    def sent(step, carry):
        tile_copy((me + step) % total).wait_send()
        return carry

    lax.fori_loop(1, total, sent, 0)


def per_device(nba, ndev, factors, amplitudes, pair_order, occ_bin, vir_bin, levels):
    owned, cols, fitting = factors.shape
    pairs, _, virt = amplitudes.shape
    window = owned * nba
    ny = 1
    while ny * ny * 4 <= nba:
        ny *= 2
    nz = nba // ny
    no = ndev // 2
    qs = fitting // nz
    nb = nz * owned
    split = window // ndev
    total = nba * ndev
    tile_c = min(cols, max(1, (4 << 20) // (nb * window * virt * 2)))
    amp_c = 16
    dims = (nz, ny, no, owned, cols, qs, window, pairs, virt, tile_c, amp_c)
    dma = pltpu.SemaphoreType.DMA
    vmem = pl.BlockSpec(memory_space=pltpu.VMEM)
    hbm = pl.BlockSpec(memory_space=pl.ANY)
    return pl.pallas_call(
        functools.partial(kernel, dims),
        out_shape=jax.ShapeDtypeStruct((owned, split * pairs), jnp.float32),
        in_specs=[hbm, hbm, vmem, vmem, vmem, vmem],
        out_specs=vmem,
        scratch_shapes=[
            pltpu.VMEM((owned, cols, fitting), jnp.bfloat16),
            pltpu.VMEM((nz, owned, ndev, cols, qs), jnp.bfloat16),
            pltpu.VMEM((ny, nz, owned, cols, qs), jnp.bfloat16),
            pltpu.VMEM((qs // LANES, window * (cols + 8), LANES), jnp.float32),
            pltpu.VMEM((cols * window, qs), jnp.bfloat16),
            pltpu.VMEM((cols // amp_c, pairs, amp_c, virt), jnp.bfloat16),
            pltpu.VMEM((virt // LANES, pairs * (amp_c + 8), LANES), jnp.float32),
            pltpu.VMEM((cols, pairs, virt), jnp.bfloat16),
            pltpu.VMEM((tile_c, nb * window, virt), jnp.bfloat16),
            pltpu.VMEM((nb, window, 2 * pairs), jnp.float32),
            pltpu.VMEM((total, owned * split, 2 * pairs), jnp.float32),
            pltpu.VMEM((total, owned * split, 2 * pairs), jnp.float32),
            dma,
            dma,
            dma((cols // amp_c,)),
            dma((nz,)),
            dma((nz, no)),
            dma((nz, no)),
            dma((nz, ny)),
            dma((nz, ndev)),
            dma((ny, nz)),
            dma((total,)),
            dma((total,)),
        ],
        compiler_params=pltpu.CompilerParams(
            collective_id=0, has_side_effects=True, vmem_limit_bytes=56 << 20
        ),
    )(
        factors,
        amplitudes,
        pair_order.reshape(1, -1),
        occ_bin.reshape(1, -1),
        vir_bin.reshape(1, -1),
        levels.reshape(1, -1),
    )


def solution(mesh):
    return jax.shard_map(
        functools.partial(per_device, mesh.shape["ba"], mesh.shape["dev"]),
        mesh=mesh,
        in_specs=(P("ba", "dev", None), P(None, "dev", None), P(), P(), P(), P()),
        out_specs=P("ba", "dev"),
        check_vma=False,
    )
```

```python
import functools

import jax
import jax.numpy as jnp
from jax import lax
from jax.experimental import pallas as pl
from jax.experimental.pallas import tpu as pltpu
from jax.sharding import PartitionSpec as P

NOCC = 8
LANES = 128
MESH = pl.DeviceIdType.MESH

level_shift = 0.3


def flip_bits(index, bits):
    result = index
    bit = 1
    while bit <= bits:
        if bits & bit:
            result = result + bit - 2 * bit * ((result // bit) % 2)
        bit *= 2
    return result


def to_column(row):
    n = row.shape[1]
    rows = lax.broadcasted_iota(jnp.int32, (n, n), 0)
    lanes = lax.broadcasted_iota(jnp.int32, (n, n), 1)
    return jnp.sum(jnp.where(rows == lanes, row, jnp.zeros_like(row)), axis=1, keepdims=True)


def kernel(
    dims,
    f_hbm,
    amps_hbm,
    order_ref,
    occ_ref,
    vir_ref,
    levels_ref,
    out_ref,
    local,
    right,
    other,
    left_f32,
    left,
    raw,
    stage,
    amps,
    ints,
    flat,
    acc,
    tiles,
    parts,
    load_sem,
    own_sem,
    amp_sem,
    send_z,
    send_o,
    send_c,
    send_y,
    recv_piece,
    recv_y,
    send_f,
    recv_f,
):
    nz, ny, no, owned, cols, qs, window, pairs, virt, tile_c, amp_c = dims
    nd = no * 2
    nb = nz * owned
    total = nz * ny * nd
    split = window // nd
    ba, dev = lax.axis_index("ba"), lax.axis_index("dev")
    me = ba * nd + dev
    z, y = ba // ny, ba % ny
    outer, core = dev // 2, dev % 2
    partner_core = outer * 2 + 1 - core
    chunks = cols // amp_c
    half, half_z = window // 2, nz // 2
    mine = z // half_z
    halves = (mine, 1 - mine)

    load = pltpu.make_async_copy(f_hbm, local, load_sem)
    load.start()
    own = pltpu.make_async_copy(
        f_hbm.at[:, :, pl.ds(pl.multiple_of(z * qs, LANES), qs)], right.at[z, :, dev], own_sem
    )
    own.start()

    def amp_load(chunk):
        return pltpu.make_async_copy(
            amps_hbm.at[:, pl.ds(chunk * amp_c, amp_c), :], raw.at[chunk], amp_sem.at[chunk]
        )

    for chunk in range(chunks):
        amp_load(chunk).start()

    barrier = pltpu.get_barrier_semaphore()

    def greet(step, carry):
        there = (me + step) % total
        pl.semaphore_signal(
            barrier, inc=1, device_id=(there // nd, there % nd), device_id_type=MESH
        )
        return carry

    lax.fori_loop(1, total, greet, 0)
    load.wait()
    own.wait()
    pl.semaphore_wait(barrier, total - 1)

    def piece_copy(piece_z, row, piece_d, send, ba_to, dev_to):
        return pltpu.make_async_remote_copy(
            src_ref=right.at[piece_z, row, piece_d],
            dst_ref=right.at[piece_z, row, piece_d],
            send_sem=send,
            recv_sem=recv_piece.at[piece_z, row, piece_d],
            device_id=(ba_to, dev_to),
            device_id_type=MESH,
        )

    def await_piece(piece_z, row, piece_d):
        piece_copy(piece_z, row, piece_d, send_z.at[0, 0], ba, partner_core).wait_recv()

    pending = []
    for step in range(1, nz):
        there = flip_bits(z, step)
        for row in range(owned):
            copy = pltpu.make_async_remote_copy(
                src_ref=local.at[row, :, pl.ds(pl.multiple_of(there * qs, LANES), qs)],
                dst_ref=right.at[z, row, dev],
                send_sem=send_z.at[step, row],
                recv_sem=recv_piece.at[z, row, dev],
                device_id=(there * ny + y, dev),
                device_id_type=MESH,
            )
            copy.start()
            pending.append(copy)

    def forward(step, row):
        from_z = flip_bits(z, step)
        if step:
            await_piece(from_z, row, dev)
        for other_outer in range(1, no):
            copy = piece_copy(
                from_z,
                row,
                dev,
                send_o.at[step, row, other_outer],
                ba,
                flip_bits(outer, other_outer) * 2 + core,
            )
            copy.start()
            pending.append(copy)
        for other_y in range(1, ny):
            copy = pltpu.make_async_remote_copy(
                src_ref=right.at[from_z, row, dev],
                dst_ref=other.at[y, from_z, row],
                send_sem=send_y.at[step, row, other_y],
                recv_sem=recv_y.at[y, from_z, row],
                device_id=(z * ny + flip_bits(y, other_y), dev),
                device_id_type=MESH,
            )
            copy.start()
            pending.append(copy)
        copy = piece_copy(from_z, row, dev, send_c.at[step, row, 0], ba, partner_core)
        copy.start()
        pending.append(copy)

    def widen(source, at_y, at_z):
        for i in range(owned):
            row = (at_z * ny + at_y) * owned + i
            base = pl.multiple_of(row * (cols + 8), 8)
            for h in range(qs // LANES):
                left_f32[h, pl.ds(base, cols), :] = source[
                    i, :, h * LANES : (h + 1) * LANES
                ].astype(jnp.float32)

    def amp_chunk(chunk):
        amp_load(chunk).wait()
        pitch = amp_c + 8

        def spread(k, carry):
            base = pl.multiple_of(k * pitch, 8)
            for h in range(virt // LANES):
                stage[h, pl.ds(base, amp_c), :] = raw[
                    chunk, k, :, h * LANES : (h + 1) * LANES
                ].astype(jnp.float32)
            return carry

        lax.fori_loop(0, pairs, spread, 0, unroll=4)

        def gather(c, carry):
            for h in range(virt // LANES):
                amps[chunk * amp_c + c, :, h * LANES : (h + 1) * LANES] = stage[
                    h, pl.ds(c, pairs, stride=pitch), :
                ].astype(jnp.bfloat16)
            return carry

        lax.fori_loop(0, amp_c, gather, 0)

    def own_rows(step):
        from_z = flip_bits(z, step)
        widen(right.at[from_z, :, dev], y, from_z)

    def collect(step):
        from_z = flip_bits(z, step)
        for row in range(owned):
            for other_outer in range(1, no):
                from_d = flip_bits(outer, other_outer) * 2 + core
                await_piece(from_z, row, from_d)
                copy = piece_copy(
                    from_z, row, from_d, send_c.at[step, row, other_outer], ba, partner_core
                )
                copy.start()
                pending.append(copy)
        for other_y in range(1, ny):
            from_y = flip_bits(y, other_y)
            for row in range(owned):
                pltpu.make_async_remote_copy(
                    src_ref=right.at[from_z, row, dev],
                    dst_ref=other.at[from_y, from_z, row],
                    send_sem=send_z.at[0, 0],
                    recv_sem=recv_y.at[from_y, from_z, row],
                    device_id=(ba, partner_core),
                    device_id_type=MESH,
                ).wait_recv()
            widen(other.at[from_y, from_z], from_y, from_z)

    def finish(step):
        from_z = flip_bits(z, step)
        for row in range(owned):
            for other_outer in range(no):
                await_piece(from_z, row, flip_bits(outer, other_outer) * 2 + 1 - core)

    def turn_half(side):
        first_row = halves[side] * half * (cols + 8)

        def turn(step, carry):
            at = step * 2
            rows = pl.ds(pl.multiple_of(at * half, 2 * half), 2 * half)
            for h in range(qs // LANES):
                left[side, rows, h * LANES : (h + 1) * LANES] = jnp.concatenate(
                    [
                        left_f32[h, pl.ds(first_row + at + i, half, stride=cols + 8), :]
                        for i in range(2)
                    ],
                    axis=0,
                ).astype(jnp.bfloat16)
            return carry

        lax.fori_loop(0, cols // 2, turn, 0, unroll=4)

    block = tile_c * half
    early = [(0, 0, j) for j in range(half_z)]
    late = [(1, side, j) for side in range(2) for j in range(half_z)] + [
        (0, 1, j) for j in range(half_z)
    ]
    height_of = owned * half

    def contract(ct, jobs, base):
        for at, (a_side, b_side, j) in enumerate(jobs):
            rows = left[a_side, pl.ds(pl.multiple_of(ct * block, block), block), :]
            from_z = halves[b_side] * half_z + j
            parts_of = []
            for i in range(owned):
                side = right[from_z, i].reshape(virt, qs)
                parts_of.append(
                    lax.dot_general(
                        rows, side, (((1,), (1,)), ((), ())), preferred_element_type=jnp.float32
                    ).reshape(tile_c, half, virt)
                )
            ints[:, at * height_of : (at + 1) * height_of, :] = jnp.concatenate(
                parts_of, axis=1
            ).astype(jnp.bfloat16)
        count = len(jobs) * height_of

        def add(t, value):
            return value + lax.dot_general(
                ints[t, 0:count, :],
                amps[ct * tile_c + t],
                (((1,), (1,)), ((), ())),
                preferred_element_type=jnp.float32,
            )

        flat[base : base + count, :] += lax.fori_loop(
            0, tile_c, add, jnp.zeros((count, pairs), jnp.float32), unroll=tile_c
        )

    flat[...] = jnp.zeros_like(flat)
    done = 0
    for step in range(half_z):
        for row in range(owned):
            forward(step, row)
            upto = (step * owned + row + 1) * chunks // (half_z * owned)
            for chunk in range(done, upto):
                amp_chunk(chunk)
            done = upto
        own_rows(step)
    for step in range(half_z, nz - 1):
        for row in range(owned):
            forward(step, row)
    for step in range(half_z):
        collect(step)
    turn_half(0)
    for step in range(half_z):
        finish(step)
    contract(0, early, 0)
    for row in range(owned):
        forward(nz - 1, row)

    def early_tile(ct, carry):
        contract(ct, early, 0)
        return carry

    lax.fori_loop(1, cols // tile_c, early_tile, 0)
    for step in range(half_z, nz):
        own_rows(step)
    for step in range(half_z, nz):
        collect(step)
    turn_half(1)
    for step in range(half_z, nz):
        finish(step)
    late_base = len(early) * height_of

    def late_tile(ct, carry):
        contract(ct, late, late_base)
        return carry

    lax.fori_loop(0, cols // tile_c, late_tile, 0)
    for at, (a_side, b_side, j) in enumerate(early + late):
        for i in range(owned):
            value = flat[at * height_of + i * half : at * height_of + (i + 1) * half, :]
            acc[
                (halves[b_side] * half_z + j) * owned + i,
                pl.ds(pl.multiple_of(halves[a_side] * half, 8), half),
                0:pairs,
            ] = value
    acc[:, :, pairs : 2 * pairs] = acc[:, :, 0:pairs]

    height = owned * split
    row_at = lax.broadcasted_iota(jnp.int32, (height, 2 * pairs), 0)
    lane_at = lax.broadcasted_iota(jnp.int32, (height, 2 * pairs), 1)

    def make_tile(there):
        to_ba, to_dev = there // nd, there % nd
        to_z, to_y = to_ba // ny, to_ba % ny
        straight = jnp.zeros((height, 2 * pairs), jnp.float32)
        pieces = []
        turned = []
        for i in range(owned):
            pieces.append(acc[to_z * owned + i, pl.ds(to_dev * split, split), :])
            for a in range(split):
                row = to_dev * split + a
                owner = row // owned
                turned.append(
                    acc[(owner // ny) * owned + row % owned, pl.ds(to_ba * owned + i, 1), :]
                )
        straight = jnp.concatenate(pieces, axis=0)
        flipped = jnp.concatenate(turned, axis=0)
        same = jnp.zeros((height, 2 * pairs), jnp.int32) + to_y == y
        owner_at = (to_dev * split + row_at % split) // owned
        return jnp.where(
            lane_at < pairs,
            jnp.where(same, straight, 0.0),
            jnp.where(owner_at % ny == y, flipped, 0.0),
        )

    def tile_copy(there):
        return pltpu.make_async_remote_copy(
            src_ref=tiles.at[there],
            dst_ref=parts.at[me],
            send_sem=send_f.at[there],
            recv_sem=recv_f.at[me],
            device_id=(there // nd, there % nd),
            device_id_type=MESH,
        )

    def send_tile(step, carry):
        there = (me + step) % total
        tiles[there] = make_tile(there)
        tile_copy(there).start()
        return carry

    lax.fori_loop(1, total, send_tile, 0)
    parts[me] = make_tile(me)

    levels = to_column(levels_ref[...])
    level_at = lax.broadcasted_iota(jnp.int32, (levels.shape[0], window), 0)
    virtual = jnp.sum(
        jnp.where(level_at == vir_ref[...], levels, 0.0), axis=0, keepdims=True
    )
    level_occ = lax.broadcasted_iota(jnp.int32, (levels.shape[0], NOCC), 0)
    occupied = to_column(
        -jnp.sum(jnp.where(level_occ == occ_ref[...], levels, 0.0), axis=0, keepdims=True)
    )
    order = order_ref[...]
    first, second = order // NOCC, order % NOCC
    occ_at = lax.broadcasted_iota(jnp.int32, (NOCC, pairs), 0)
    pair_energy = jnp.sum(
        jnp.where(occ_at == first, occupied, 0.0), axis=0, keepdims=True
    ) + jnp.sum(jnp.where(occ_at == second, occupied, 0.0), axis=0, keepdims=True)
    win_row = lax.broadcasted_iota(jnp.int32, (height, window), 0)
    win_lane = lax.broadcasted_iota(jnp.int32, (height, window), 1)
    right_energy = jnp.sum(
        jnp.where(win_lane == ba * owned + win_row // split, virtual, 0.0), axis=1, keepdims=True
    )
    left_energy = jnp.sum(
        jnp.where(win_lane == dev * split + win_row % split, virtual, 0.0), axis=1, keepdims=True
    )
    denominator = right_energy + left_energy - pair_energy + level_shift
    permuter = (to_column(order) == second * NOCC + first).astype(jnp.float32)

    def arrive(step, carry):
        there = (me + step) % total
        pltpu.make_async_remote_copy(
            src_ref=tiles.at[there],
            dst_ref=parts.at[there],
            send_sem=send_f.at[there],
            recv_sem=recv_f.at[there],
            device_id=(there // nd, there % nd),
            device_id_type=MESH,
        ).wait_recv()
        return carry

    lax.fori_loop(1, total, arrive, 0)
    summed = jnp.sum(parts[...], axis=0)
    moved = jnp.dot(
        summed[:, pairs:],
        permuter,
        precision=lax.Precision.HIGHEST,
        preferred_element_type=jnp.float32,
    )
    result = (summed[:, :pairs] + moved) / denominator
    for i in range(owned):
        for a in range(split):
            out_ref[i : i + 1, a * pairs : (a + 1) * pairs] = result[
                i * split + a : i * split + a + 1, :
            ]

    for copy in pending:
        copy.wait_send()

    def sent(step, carry):
        tile_copy((me + step) % total).wait_send()
        return carry

    lax.fori_loop(1, total, sent, 0)


def per_device(nba, ndev, factors, amplitudes, pair_order, occ_bin, vir_bin, levels):
    owned, cols, fitting = factors.shape
    pairs, _, virt = amplitudes.shape
    window = owned * nba
    ny = 1
    while ny * ny * 4 <= nba:
        ny *= 2
    nz = nba // ny
    no = ndev // 2
    qs = fitting // nz
    nb = nz * owned
    split = window // ndev
    total = nba * ndev
    tile_c = min(cols, max(1, (4 << 20) // (nb * window * virt * 2)))
    amp_c = 16
    dims = (nz, ny, no, owned, cols, qs, window, pairs, virt, tile_c, amp_c)
    dma = pltpu.SemaphoreType.DMA
    vmem = pl.BlockSpec(memory_space=pltpu.VMEM)
    hbm = pl.BlockSpec(memory_space=pl.ANY)
    return pl.pallas_call(
        functools.partial(kernel, dims),
        out_shape=jax.ShapeDtypeStruct((owned, split * pairs), jnp.float32),
        in_specs=[hbm, hbm, vmem, vmem, vmem, vmem],
        out_specs=vmem,
        scratch_shapes=[
            pltpu.VMEM((owned, cols, fitting), jnp.bfloat16),
            pltpu.VMEM((nz, owned, ndev, cols, qs), jnp.bfloat16),
            pltpu.VMEM((ny, nz, owned, cols, qs), jnp.bfloat16),
            pltpu.VMEM((qs // LANES, window * (cols + 8), LANES), jnp.float32),
            pltpu.VMEM((2, cols * window // 2, qs), jnp.bfloat16),
            pltpu.VMEM((cols // amp_c, pairs, amp_c, virt), jnp.bfloat16),
            pltpu.VMEM((virt // LANES, pairs * (amp_c + 8), LANES), jnp.float32),
            pltpu.VMEM((cols, pairs, virt), jnp.bfloat16),
            pltpu.VMEM((tile_c, nb * window, virt), jnp.bfloat16),
            pltpu.VMEM((nb * window, pairs), jnp.float32),
            pltpu.VMEM((nb, window, 2 * pairs), jnp.float32),
            pltpu.VMEM((total, owned * split, 2 * pairs), jnp.float32),
            pltpu.VMEM((total, owned * split, 2 * pairs), jnp.float32),
            dma,
            dma,
            dma((cols // amp_c,)),
            dma((nz, owned)),
            dma((nz, owned, no)),
            dma((nz, owned, no)),
            dma((nz, owned, ny)),
            dma((nz, owned, ndev)),
            dma((ny, nz, owned)),
            dma((total,)),
            dma((total,)),
        ],
        compiler_params=pltpu.CompilerParams(
            collective_id=0, has_side_effects=True, vmem_limit_bytes=56 << 20
        ),
    )(
        factors,
        amplitudes,
        pair_order.reshape(1, -1),
        occ_bin.reshape(1, -1),
        vir_bin.reshape(1, -1),
        levels.reshape(1, -1),
    )


def solution(mesh):
    return jax.shard_map(
        functools.partial(per_device, mesh.shape["ba"], mesh.shape["dev"]),
        mesh=mesh,
        in_specs=(P("ba", "dev", None), P(None, "dev", None), P(), P(), P(), P()),
        out_specs=P("ba", "dev"),
        check_vma=False,
    )
```

```python
import functools

import jax
import jax.numpy as jnp
from jax import lax
from jax.experimental import pallas as pl
from jax.experimental.pallas import tpu as pltpu
from jax.sharding import PartitionSpec as P

NOCC = 8
LANES = 128
MESH = pl.DeviceIdType.MESH

level_shift = 0.3


def flip_bits(index, bits):
    result = index
    bit = 1
    while bit <= bits:
        if bits & bit:
            result = result + bit - 2 * bit * ((result // bit) % 2)
        bit *= 2
    return result


def to_column(row):
    n = row.shape[1]
    rows = lax.broadcasted_iota(jnp.int32, (n, n), 0)
    lanes = lax.broadcasted_iota(jnp.int32, (n, n), 1)
    return jnp.sum(jnp.where(rows == lanes, row, jnp.zeros_like(row)), axis=1, keepdims=True)


def kernel(
    dims,
    f_hbm,
    amps_hbm,
    order_ref,
    occ_ref,
    vir_ref,
    levels_ref,
    out_ref,
    local,
    right,
    other,
    left_f32,
    left,
    raw,
    stage,
    amps,
    ints,
    flat,
    acc,
    tiles,
    parts,
    load_sem,
    own_sem,
    amp_sem,
    send_z,
    send_o,
    send_c,
    send_y,
    recv_piece,
    recv_y,
    send_f,
    recv_f,
):
    nz, ny, no, owned, cols, qs, window, pairs, virt, tile_c, amp_c = dims
    nd = no * 2
    nb = nz * owned
    total = nz * ny * nd
    split = window // nd
    ba, dev = lax.axis_index("ba"), lax.axis_index("dev")
    me = ba * nd + dev
    z, y = ba // ny, ba % ny
    outer, core = dev // 2, dev % 2
    partner_core = outer * 2 + 1 - core
    chunks = cols // amp_c
    half, half_z = window // 2, nz // 2
    mine = z // half_z
    halves = (mine, 1 - mine)

    load = pltpu.make_async_copy(f_hbm, local, load_sem)
    load.start()
    own = pltpu.make_async_copy(
        f_hbm.at[:, :, pl.ds(pl.multiple_of(z * qs, LANES), qs)], right.at[z, :, dev], own_sem
    )
    own.start()

    def amp_load(chunk):
        return pltpu.make_async_copy(
            amps_hbm.at[:, pl.ds(chunk * amp_c, amp_c), :], raw.at[chunk], amp_sem.at[chunk]
        )

    for chunk in range(chunks):
        amp_load(chunk).start()

    barrier = pltpu.get_barrier_semaphore()

    def greet(step, carry):
        there = (me + step) % total
        pl.semaphore_signal(
            barrier, inc=1, device_id=(there // nd, there % nd), device_id_type=MESH
        )
        return carry

    lax.fori_loop(1, total, greet, 0)
    load.wait()
    own.wait()
    pl.semaphore_wait(barrier, total - 1)

    def piece_copy(piece_z, row, piece_d, send, ba_to, dev_to):
        return pltpu.make_async_remote_copy(
            src_ref=right.at[piece_z, row, piece_d],
            dst_ref=right.at[piece_z, row, piece_d],
            send_sem=send,
            recv_sem=recv_piece.at[piece_z, row, piece_d],
            device_id=(ba_to, dev_to),
            device_id_type=MESH,
        )

    def await_piece(piece_z, row, piece_d):
        piece_copy(piece_z, row, piece_d, send_z.at[0, 0], ba, partner_core).wait_recv()

    pending = []
    for step in range(1, nz):
        there = flip_bits(z, step)
        for row in range(owned):
            copy = pltpu.make_async_remote_copy(
                src_ref=local.at[row, :, pl.ds(pl.multiple_of(there * qs, LANES), qs)],
                dst_ref=right.at[z, row, dev],
                send_sem=send_z.at[step, row],
                recv_sem=recv_piece.at[z, row, dev],
                device_id=(there * ny + y, dev),
                device_id_type=MESH,
            )
            copy.start()
            pending.append(copy)

    def forward(step, row):
        from_z = flip_bits(z, step)
        if step:
            await_piece(from_z, row, dev)
        for other_outer in range(1, no):
            copy = piece_copy(
                from_z,
                row,
                dev,
                send_o.at[step, row, other_outer],
                ba,
                flip_bits(outer, other_outer) * 2 + core,
            )
            copy.start()
            pending.append(copy)
        for other_y in range(1, ny):
            copy = pltpu.make_async_remote_copy(
                src_ref=right.at[from_z, row, dev],
                dst_ref=other.at[y, from_z, row],
                send_sem=send_y.at[step, row, other_y],
                recv_sem=recv_y.at[y, from_z, row],
                device_id=(z * ny + flip_bits(y, other_y), dev),
                device_id_type=MESH,
            )
            copy.start()
            pending.append(copy)
        copy = piece_copy(from_z, row, dev, send_c.at[step, row, 0], ba, partner_core)
        copy.start()
        pending.append(copy)

    def widen(source, at_y, at_z):
        for i in range(owned):
            row = (at_z * ny + at_y) * owned + i
            base = pl.multiple_of(row * (cols + 8), 8)
            for h in range(qs // LANES):
                left_f32[h, pl.ds(base, cols), :] = source[
                    i, :, h * LANES : (h + 1) * LANES
                ].astype(jnp.float32)

    def amp_chunk(chunk):
        amp_load(chunk).wait()
        pitch = amp_c + 8

        def spread(k, carry):
            base = pl.multiple_of(k * pitch, 8)
            for h in range(virt // LANES):
                stage[h, pl.ds(base, amp_c), :] = raw[
                    chunk, k, :, h * LANES : (h + 1) * LANES
                ].astype(jnp.float32)
            return carry

        lax.fori_loop(0, pairs, spread, 0, unroll=4)

        def gather(c, carry):
            for h in range(virt // LANES):
                amps[chunk * amp_c + c, :, h * LANES : (h + 1) * LANES] = stage[
                    h, pl.ds(c, pairs, stride=pitch), :
                ].astype(jnp.bfloat16)
            return carry

        lax.fori_loop(0, amp_c, gather, 0)

    def own_rows(step):
        from_z = flip_bits(z, step)
        widen(right.at[from_z, :, dev], y, from_z)

    def collect(step):
        from_z = flip_bits(z, step)
        for row in range(owned):
            for other_outer in range(1, no):
                from_d = flip_bits(outer, other_outer) * 2 + core
                await_piece(from_z, row, from_d)
                copy = piece_copy(
                    from_z, row, from_d, send_c.at[step, row, other_outer], ba, partner_core
                )
                copy.start()
                pending.append(copy)
        for other_y in range(1, ny):
            from_y = flip_bits(y, other_y)
            for row in range(owned):
                pltpu.make_async_remote_copy(
                    src_ref=right.at[from_z, row, dev],
                    dst_ref=other.at[from_y, from_z, row],
                    send_sem=send_z.at[0, 0],
                    recv_sem=recv_y.at[from_y, from_z, row],
                    device_id=(ba, partner_core),
                    device_id_type=MESH,
                ).wait_recv()
            widen(other.at[from_y, from_z], from_y, from_z)

    def finish(step):
        from_z = flip_bits(z, step)
        for row in range(owned):
            for other_outer in range(no):
                await_piece(from_z, row, flip_bits(outer, other_outer) * 2 + 1 - core)

    def turn_half(side):
        first_row = halves[side] * half * (cols + 8)

        def turn(step, carry):
            at = step * 2
            rows = pl.ds(pl.multiple_of(at * half, 2 * half), 2 * half)
            for h in range(qs // LANES):
                left[side, rows, h * LANES : (h + 1) * LANES] = jnp.concatenate(
                    [
                        left_f32[h, pl.ds(first_row + at + i, half, stride=cols + 8), :]
                        for i in range(2)
                    ],
                    axis=0,
                ).astype(jnp.bfloat16)
            return carry

        lax.fori_loop(0, cols // 2, turn, 0, unroll=4)

    block = tile_c * half
    early = [(0, 0, j) for j in range(half_z)]
    late = [(1, side, j) for side in range(2) for j in range(half_z)] + [
        (0, 1, j) for j in range(half_z)
    ]
    height_of = owned * half

    def contract(ct, jobs, base):
        for at, (a_side, b_side, j) in enumerate(jobs):
            rows = left[a_side, pl.ds(pl.multiple_of(ct * block, block), block), :]
            from_z = halves[b_side] * half_z + j
            parts_of = []
            for i in range(owned):
                side = right[from_z, i].reshape(virt, qs)
                parts_of.append(
                    lax.dot_general(
                        rows, side, (((1,), (1,)), ((), ())), preferred_element_type=jnp.float32
                    ).reshape(tile_c, half, virt)
                )
            ints[:, at * height_of : (at + 1) * height_of, :] = jnp.concatenate(
                parts_of, axis=1
            ).astype(jnp.bfloat16)
        count = len(jobs) * height_of

        def add(t, value):
            return value + lax.dot_general(
                ints[t, 0:count, :],
                amps[ct * tile_c + t],
                (((1,), (1,)), ((), ())),
                preferred_element_type=jnp.float32,
            )

        flat[base : base + count, :] += lax.fori_loop(
            0, tile_c, add, jnp.zeros((count, pairs), jnp.float32), unroll=tile_c
        )

    flat[...] = jnp.zeros_like(flat)
    done = 0
    for step in range(half_z):
        for row in range(owned):
            forward(step, row)
            upto = (step * owned + row + 1) * chunks // (half_z * owned)
            for chunk in range(done, upto):
                amp_chunk(chunk)
            done = upto
        own_rows(step)
    for step in range(half_z, nz - 1):
        for row in range(owned):
            forward(step, row)
    for step in range(half_z):
        collect(step)
    turn_half(0)
    for step in range(half_z):
        finish(step)
    for row in range(owned):
        forward(nz - 1, row)

    def early_tile(ct, carry):
        contract(ct, early, 0)
        return carry

    lax.fori_loop(0, cols // tile_c, early_tile, 0)
    for step in range(half_z, nz):
        own_rows(step)
    for step in range(half_z, nz):
        collect(step)
    turn_half(1)
    for step in range(half_z, nz):
        finish(step)
    late_base = len(early) * height_of

    def late_tile(ct, carry):
        contract(ct, late, late_base)
        return carry

    lax.fori_loop(0, cols // tile_c, late_tile, 0)
    for at, (a_side, b_side, j) in enumerate(early + late):
        for i in range(owned):
            value = flat[at * height_of + i * half : at * height_of + (i + 1) * half, :]
            acc[
                (halves[b_side] * half_z + j) * owned + i,
                pl.ds(pl.multiple_of(halves[a_side] * half, 8), half),
                0:pairs,
            ] = value
    acc[:, :, pairs : 2 * pairs] = acc[:, :, 0:pairs]

    height = owned * split
    row_at = lax.broadcasted_iota(jnp.int32, (height, 2 * pairs), 0)
    lane_at = lax.broadcasted_iota(jnp.int32, (height, 2 * pairs), 1)

    def make_tile(there):
        to_ba, to_dev = there // nd, there % nd
        to_z, to_y = to_ba // ny, to_ba % ny
        straight = jnp.zeros((height, 2 * pairs), jnp.float32)
        pieces = []
        turned = []
        for i in range(owned):
            pieces.append(acc[to_z * owned + i, pl.ds(to_dev * split, split), :])
            for a in range(split):
                row = to_dev * split + a
                owner = row // owned
                turned.append(
                    acc[(owner // ny) * owned + row % owned, pl.ds(to_ba * owned + i, 1), :]
                )
        straight = jnp.concatenate(pieces, axis=0)
        flipped = jnp.concatenate(turned, axis=0)
        same = jnp.zeros((height, 2 * pairs), jnp.int32) + to_y == y
        owner_at = (to_dev * split + row_at % split) // owned
        return jnp.where(
            lane_at < pairs,
            jnp.where(same, straight, 0.0),
            jnp.where(owner_at % ny == y, flipped, 0.0),
        )

    def tile_copy(there):
        return pltpu.make_async_remote_copy(
            src_ref=tiles.at[there],
            dst_ref=parts.at[me],
            send_sem=send_f.at[there],
            recv_sem=recv_f.at[me],
            device_id=(there // nd, there % nd),
            device_id_type=MESH,
        )

    def send_tile(step, carry):
        there = (me + step) % total
        tiles[there] = make_tile(there)
        tile_copy(there).start()
        return carry

    lax.fori_loop(1, total, send_tile, 0)
    parts[me] = make_tile(me)

    levels = to_column(levels_ref[...])
    level_at = lax.broadcasted_iota(jnp.int32, (levels.shape[0], window), 0)
    virtual = jnp.sum(
        jnp.where(level_at == vir_ref[...], levels, 0.0), axis=0, keepdims=True
    )
    level_occ = lax.broadcasted_iota(jnp.int32, (levels.shape[0], NOCC), 0)
    occupied = to_column(
        -jnp.sum(jnp.where(level_occ == occ_ref[...], levels, 0.0), axis=0, keepdims=True)
    )
    order = order_ref[...]
    first, second = order // NOCC, order % NOCC
    occ_at = lax.broadcasted_iota(jnp.int32, (NOCC, pairs), 0)
    pair_energy = jnp.sum(
        jnp.where(occ_at == first, occupied, 0.0), axis=0, keepdims=True
    ) + jnp.sum(jnp.where(occ_at == second, occupied, 0.0), axis=0, keepdims=True)
    win_row = lax.broadcasted_iota(jnp.int32, (height, window), 0)
    win_lane = lax.broadcasted_iota(jnp.int32, (height, window), 1)
    right_energy = jnp.sum(
        jnp.where(win_lane == ba * owned + win_row // split, virtual, 0.0), axis=1, keepdims=True
    )
    left_energy = jnp.sum(
        jnp.where(win_lane == dev * split + win_row % split, virtual, 0.0), axis=1, keepdims=True
    )
    denominator = right_energy + left_energy - pair_energy + level_shift
    permuter = (to_column(order) == second * NOCC + first).astype(jnp.float32)

    def arrive(step, carry):
        there = (me + step) % total
        pltpu.make_async_remote_copy(
            src_ref=tiles.at[there],
            dst_ref=parts.at[there],
            send_sem=send_f.at[there],
            recv_sem=recv_f.at[there],
            device_id=(there // nd, there % nd),
            device_id_type=MESH,
        ).wait_recv()
        return carry

    lax.fori_loop(1, total, arrive, 0)
    summed = jnp.sum(parts[...], axis=0)
    moved = jnp.dot(
        summed[:, pairs:],
        permuter,
        precision=lax.Precision.HIGHEST,
        preferred_element_type=jnp.float32,
    )
    result = (summed[:, :pairs] + moved) / denominator
    for i in range(owned):
        for a in range(split):
            out_ref[i : i + 1, a * pairs : (a + 1) * pairs] = result[
                i * split + a : i * split + a + 1, :
            ]

    for copy in pending:
        copy.wait_send()

    def sent(step, carry):
        tile_copy((me + step) % total).wait_send()
        return carry

    lax.fori_loop(1, total, sent, 0)


def per_device(nba, ndev, factors, amplitudes, pair_order, occ_bin, vir_bin, levels):
    owned, cols, fitting = factors.shape
    pairs, _, virt = amplitudes.shape
    window = owned * nba
    ny = 1
    while ny * ny * 4 <= nba:
        ny *= 2
    nz = nba // ny
    no = ndev // 2
    qs = fitting // nz
    nb = nz * owned
    split = window // ndev
    total = nba * ndev
    tile_c = min(cols, max(1, (4 << 20) // (nb * window * virt * 2)))
    amp_c = 16
    dims = (nz, ny, no, owned, cols, qs, window, pairs, virt, tile_c, amp_c)
    dma = pltpu.SemaphoreType.DMA
    vmem = pl.BlockSpec(memory_space=pltpu.VMEM)
    hbm = pl.BlockSpec(memory_space=pl.ANY)
    return pl.pallas_call(
        functools.partial(kernel, dims),
        out_shape=jax.ShapeDtypeStruct((owned, split * pairs), jnp.float32),
        in_specs=[hbm, hbm, vmem, vmem, vmem, vmem],
        out_specs=vmem,
        scratch_shapes=[
            pltpu.VMEM((owned, cols, fitting), jnp.bfloat16),
            pltpu.VMEM((nz, owned, ndev, cols, qs), jnp.bfloat16),
            pltpu.VMEM((ny, nz, owned, cols, qs), jnp.bfloat16),
            pltpu.VMEM((qs // LANES, window * (cols + 8), LANES), jnp.float32),
            pltpu.VMEM((2, cols * window // 2, qs), jnp.bfloat16),
            pltpu.VMEM((cols // amp_c, pairs, amp_c, virt), jnp.bfloat16),
            pltpu.VMEM((virt // LANES, pairs * (amp_c + 8), LANES), jnp.float32),
            pltpu.VMEM((cols, pairs, virt), jnp.bfloat16),
            pltpu.VMEM((tile_c, nb * window, virt), jnp.bfloat16),
            pltpu.VMEM((nb * window, pairs), jnp.float32),
            pltpu.VMEM((nb, window, 2 * pairs), jnp.float32),
            pltpu.VMEM((total, owned * split, 2 * pairs), jnp.float32),
            pltpu.VMEM((total, owned * split, 2 * pairs), jnp.float32),
            dma,
            dma,
            dma((cols // amp_c,)),
            dma((nz, owned)),
            dma((nz, owned, no)),
            dma((nz, owned, no)),
            dma((nz, owned, ny)),
            dma((nz, owned, ndev)),
            dma((ny, nz, owned)),
            dma((total,)),
            dma((total,)),
        ],
        compiler_params=pltpu.CompilerParams(
            collective_id=0, has_side_effects=True, vmem_limit_bytes=56 << 20
        ),
    )(
        factors,
        amplitudes,
        pair_order.reshape(1, -1),
        occ_bin.reshape(1, -1),
        vir_bin.reshape(1, -1),
        levels.reshape(1, -1),
    )


def solution(mesh):
    return jax.shard_map(
        functools.partial(per_device, mesh.shape["ba"], mesh.shape["dev"]),
        mesh=mesh,
        in_specs=(P("ba", "dev", None), P(None, "dev", None), P(), P(), P(), P()),
        out_specs=P("ba", "dev"),
        check_vma=False,
    )
```
